32 devices in a mesh: ens: 1 (over z), sp: 32 (over y, x, core).
Axes of the slice: x: 4, y: 4, z: 1, core: 2. Of those that a mesh axis runs over, the one named last changes fastest.
The devices are a block of a 4x4x8 slice.
Arguments:
- x_seq: bfloat16 [16384, 512], P(('ens', 'sp'))
- w_past: bfloat16 [3, 10, 512, 1024], replicated
- w_now: bfloat16 [3, 10, 512, 1024], replicated
- b_conv: float32 [3, 10, 1024], replicated
- w_res: bfloat16 [3, 10, 512, 512], replicated
- w_skip: bfloat16 [3, 10, 512, 256], replicated
- w_out1: bfloat16 [256, 256], replicated
- b_out1: float32 [256], replicated
- w_out2: bfloat16 [256, 256], replicated
- b_out2: float32 [256], replicated
Outputs:
- output 1: float32 [16384, 256], P(('ens', 'sp'))
- output 2: bfloat16 [16384, 512], P(('ens', 'sp'))
All inputs are finite; a program needn't handle non-finite values.
Results may differ from the reference program's by a relative error of at most 0.02.
Values are sent between devices in bfloat16 or wider.
A program may use at most 768 MiB of HBM per device.

```python
import jax
import jax.numpy as jnp
from jax import lax

SEQ_LEN = 16384
RES_CH = 512
GATE_CH = 512
SKIP_CH = 256
CLASSES = 256
DIL_CYCLE = 10
STACKS = 3
LAYERS_ALL = STACKS * DIL_CYCLE


def setup_inputs(seed: int = 0, part: int = 0) -> dict:
    root_key = jax.random.key(seed)
    subkeys = jax.random.split(root_key, 10)
    seq_key = jax.random.fold_in(subkeys[0], part)
    conv_shape = (STACKS, DIL_CYCLE, RES_CH, 2 * GATE_CH)
    conv_scale = (2 * RES_CH) ** -0.5
    proj_scale = 2.0 * (GATE_CH * LAYERS_ALL) ** -0.5
    head_scale = 2.0 * SKIP_CH ** -0.5
    x_seq = jax.random.normal(seq_key, (SEQ_LEN, RES_CH), jnp.float32)
    w_past = jax.random.normal(subkeys[1], conv_shape, jnp.float32) * conv_scale
    w_now = jax.random.normal(subkeys[2], conv_shape, jnp.float32) * conv_scale
    b_conv = jax.random.normal(subkeys[3], (STACKS, DIL_CYCLE, 2 * GATE_CH), jnp.float32) * 0.5
    w_res = jax.random.normal(subkeys[4], (STACKS, DIL_CYCLE, GATE_CH, RES_CH), jnp.float32) * proj_scale
    w_skip = jax.random.normal(subkeys[5], (STACKS, DIL_CYCLE, GATE_CH, SKIP_CH), jnp.float32) * proj_scale
    w_out1 = jax.random.normal(subkeys[6], (SKIP_CH, SKIP_CH), jnp.float32) * head_scale
    b_out1 = jax.random.normal(subkeys[7], (SKIP_CH,), jnp.float32) * 0.5
    w_out2 = jax.random.normal(subkeys[8], (SKIP_CH, CLASSES), jnp.float32) * head_scale
    b_out2 = jax.random.normal(subkeys[9], (CLASSES,), jnp.float32) * 0.5
    return {
        "x_seq": x_seq.astype(jnp.bfloat16),
        "w_past": w_past.astype(jnp.bfloat16),
        "w_now": w_now.astype(jnp.bfloat16),
        "b_conv": b_conv,
        "w_res": w_res.astype(jnp.bfloat16),
        "w_skip": w_skip.astype(jnp.bfloat16),
        "w_out1": w_out1.astype(jnp.bfloat16),
        "b_out1": b_out1,
        "w_out2": w_out2.astype(jnp.bfloat16),
        "b_out2": b_out2,
    }


def reference(x_seq, w_past, w_now, b_conv, w_res, w_skip, w_out1, b_out1, w_out2, b_out2):
    def stack_body(carry, stack_w):
        hidden, skip_sum = carry
        past_w, now_w, conv_b, res_w, skip_w = stack_w
        for layer_pos in range(DIL_CYCLE):
            dilation = 2 ** layer_pos
            shifted = jnp.concatenate([jnp.zeros((dilation, RES_CH), hidden.dtype), hidden[:SEQ_LEN - dilation]], axis=0)
            pre_act = (jnp.dot(shifted, past_w[layer_pos], preferred_element_type=jnp.float32)
                       + jnp.dot(hidden, now_w[layer_pos], preferred_element_type=jnp.float32)
                       + conv_b[layer_pos])
            gated = (jnp.tanh(pre_act[:, :GATE_CH]) * jax.nn.sigmoid(pre_act[:, GATE_CH:])).astype(jnp.bfloat16)
            hidden = (hidden.astype(jnp.float32) + jnp.dot(gated, res_w[layer_pos], preferred_element_type=jnp.float32)).astype(jnp.bfloat16)
            skip_sum = skip_sum + jnp.dot(gated, skip_w[layer_pos], preferred_element_type=jnp.float32)
        return (hidden, skip_sum), None

    skip_init = jnp.zeros((SEQ_LEN, SKIP_CH), jnp.float32)
    (hidden, skip_sum), _ = lax.scan(stack_body, (x_seq, skip_init), (w_past, w_now, b_conv, w_res, w_skip))
    skip_act = jax.nn.relu(skip_sum).astype(jnp.bfloat16)
    mid_act = jax.nn.relu(jnp.dot(skip_act, w_out1, preferred_element_type=jnp.float32) + b_out1).astype(jnp.bfloat16)
    logits = jnp.dot(mid_act, w_out2, preferred_element_type=jnp.float32) + b_out2
    return (logits, hidden)
```

```python
import functools

import jax
import jax.numpy as jnp
from jax import lax
from jax.experimental import pallas as pl
from jax.experimental.pallas import tpu as pltpu
from jax.sharding import PartitionSpec as P

TILE = 16
ROWS = 128
CHUNK = 256
MESH = pl.DeviceIdType.MESH


def halo_rows(k):
    return max(TILE, 2 ** k)


def wavenet_kernel(n_sp, stacks, cycle, x_ref, wp_ref, wn_ref, b_ref, wr_ref, ws_ref, w1_ref, c1_ref, w2_ref, c2_ref,
                   y_ref, hout_ref, hbuf, skip, wp, wn, wr, ws, stage, *scratch):
    halos, (x_sem, w_sem, send_sem, recv_sem, out_sem) = scratch[:cycle], scratch[cycle:]
    me = lax.axis_index("sp")
    ens = lax.axis_index("ens")
    right = lax.rem(me + 1, n_sp)
    left = lax.rem(me + n_sp - 1, n_sp)
    first = me == 0
    rows = hbuf.shape[0]
    gate = wr.shape[1]
    f32, bf16 = jnp.float32, jnp.bfloat16

    def weight_copies(stack, k):
        return [pltpu.make_async_copy(src.at[stack, k], dst.at[k], w_sem.at[k, i])
                for i, (src, dst) in enumerate(((wp_ref, wp), (wn_ref, wn), (wr_ref, wr), (ws_ref, ws)))]

    def pieces(k):
        lo = rows - halo_rows(k)
        out = []
        hi = rows
        while hi > lo:
            out.append((max(lo, hi - ROWS), hi))
            hi = max(lo, hi - ROWS)
        return out

    stage_off = []
    off = 0
    for k in range(cycle):
        stage_off.append(off)
        off += halo_rows(k)

    def send(stack, k, p):
        a, b = pieces(k)[p]
        lo = rows - halo_rows(k)
        return pltpu.make_async_remote_copy(
            src_ref=stage.at[pl.ds(stage_off[k] + a - lo, b - a)],
            dst_ref=halos[k].at[stack, pl.ds(a - lo, b - a)],
            send_sem=send_sem.at[k, p],
            recv_sem=recv_sem.at[stack, k, p],
            device_id=(ens, right),
            device_id_type=MESH,
        )

    x_copy = pltpu.make_async_copy(x_ref, hbuf, x_sem)
    x_copy.start()
    for k in range(cycle):
        for c in weight_copies(0, k):
            c.start()

    barrier = pltpu.get_barrier_semaphore()
    for other in (left, right):
        pl.semaphore_signal(barrier, inc=1, device_id=(ens, other), device_id_type=MESH)
    pl.semaphore_wait(barrier, 2)

    skip[...] = jnp.zeros_like(skip)
    x_copy.wait()

    blocks = [(r, r + ROWS) for r in range(rows - ROWS, -1, -ROWS)]
    units = [(k, r0, r1) for k in range(cycle) for (r0, r1) in blocks]

    def past_rows(stack, k, r0, r1):
        d = 2 ** k
        if d >= rows:
            return jnp.where(first, jnp.zeros((), bf16), halos[k][stack, r0:r1, :])
        if d >= TILE:
            a, b = r0 - d, r1 - d
            parts = []
            if a < 0:
                h = halo_rows(k)
                v = halos[k][stack, h + a:h + min(b, 0), :]
                parts.append(jnp.where(first, jnp.zeros((), bf16), v))
            if b > 0:
                parts.append(hbuf[max(a, 0):b, :])
            return parts[0] if len(parts) == 1 else jnp.concatenate(parts, axis=0)
        if r0 == 0:
            v = jnp.concatenate([jnp.where(first, jnp.zeros((), bf16), halos[k][stack]), hbuf[0:r1, :]], axis=0)
        else:
            v = hbuf[r0 - TILE:r1, :]
        v = v.astype(f32)[TILE - d:TILE - d + r1 - r0]
        return v.astype(bf16)

    def body(stack, carry):
        waited_w = set()
        waited_h = set()

        def conv(unit):
            k, r0, r1 = unit
            if k not in waited_w:
                waited_w.add(k)
                for c in weight_copies(stack, k):
                    c.wait()
            lo = rows - halo_rows(k)
            d = 2 ** k
            for p, (a, b) in enumerate(pieces(k)):
                need = (r0 - d < b - rows) and (r1 - d > a - rows)
                if need and (k, p) not in waited_h:
                    waited_h.add((k, p))
                    send(stack, k, p).wait_recv()
            past = past_rows(stack, k, r0, r1)
            now = hbuf[r0:r1, :]
            return past, now

        def conv_chunk(unit, lhs, c):
            k = unit[0]
            past, now = lhs
            out = []
            for base in (c * CHUNK, gate + c * CHUNK):
                z = jnp.dot(past, wp[k, :, base:base + CHUNK], preferred_element_type=f32)
                z = z + jnp.dot(now, wn[k, :, base:base + CHUNK], preferred_element_type=f32)
                out.append(z)
            return out

        def gated(unit, z, c):
            k = unit[0]
            bias = b_ref[stack, k]
            zt = z[0] + bias[None, c * CHUNK:(c + 1) * CHUNK]
            zs = z[1] + bias[None, gate + c * CHUNK:gate + (c + 1) * CHUNK]
            sig = 0.5 * jnp.tanh(0.5 * zs) + 0.5
            return (jnp.tanh(zt) * sig).astype(bf16)

        def finish(unit, g):
            k, r0, r1 = unit
            g = jnp.concatenate(g, axis=1)
            h = hbuf[r0:r1, :].astype(f32) + jnp.dot(g, wr[k], preferred_element_type=f32)
            h = h.astype(bf16)
            hbuf[r0:r1, :] = h
            skip[r0:r1, :] += jnp.dot(g, ws[k], preferred_element_type=f32)
            nk = k + 1
            nstack = stack
            if nk == cycle:
                nk = 0
            lo = rows - halo_rows(nk)
            todo = [(p, a, b) for p, (a, b) in enumerate(pieces(nk)) if a >= r0 and b <= r1]

            def go():
                for p, a, b in todo:
                    o = stage_off[nk] + a - lo
                    send_done(nk, p)
                    stage[o:o + b - a, :] = h[a - r0:b - r0]
                    send(stack + (1 if k + 1 == cycle else 0), nk, p).start()

            def send_done(nk, p):
                if nk == 0:
                    send(stack, nk, p).wait_send()

            if todo:
                if k + 1 == cycle:
                    pl.when(stack < stacks - 1)(go)
                else:
                    go()

        prev = None
        for u in units + [None]:
            if u is not None:
                lhs = conv(u)
            znew, g = [], []
            for c in range(gate // CHUNK):
                if u is not None:
                    znew.append(conv_chunk(u, lhs, c))
                if prev is not None:
                    g.append(gated(prev[0], prev[1][c], c))
            if prev is not None:
                finish(prev[0], g)
                k, r0, _ = prev[0]
                if r0 == 0 and (k == cycle // 2 - 1 or k == cycle - 1):
                    @pl.when(stack < stacks - 1)
                    def _():
                        for kk in range(0 if k < cycle // 2 else cycle // 2, k + 1):
                            for cp in weight_copies(stack + 1, kk):
                                cp.start()
            prev = (u, znew)
        for k in range(1, cycle):
            for p in range(len(pieces(k))):
                send(stack, k, p).wait_send()
        return carry

    lo = rows - halo_rows(0)
    stage[0:halo_rows(0), :] = hbuf[lo:rows, :]
    send(0, 0, 0).start()
    lax.fori_loop(0, stacks, body, 0)
    send(stacks - 1, 0, 0).wait_send()

    h_copy = pltpu.make_async_copy(hbuf, hout_ref, out_sem.at[0])
    h_copy.start()
    a = jnp.maximum(skip[...], 0.0).astype(bf16)
    m = jnp.dot(a, w1_ref[...], preferred_element_type=f32) + c1_ref[...]
    m = jnp.maximum(m, 0.0).astype(bf16)
    skip[...] = jnp.dot(m, w2_ref[...], preferred_element_type=f32) + c2_ref[...]
    y_copy = pltpu.make_async_copy(skip, y_ref, out_sem.at[1])
    y_copy.start()
    h_copy.wait()
    y_copy.wait()


def solution(mesh):
    n_sp = mesh.shape["sp"]
    row_spec = P(("ens", "sp"), None)

    def local_stack(x_seq, w_past, w_now, b_conv, w_res, w_skip, w_out1, b_out1, w_out2, b_out2):
        rows, res_ch = x_seq.shape
        stacks, cycle = w_past.shape[:2]
        skip_ch = w_skip.shape[-1]
        gate = w_res.shape[2]
        max_pieces = max(1, 2 ** (cycle - 1) // ROWS)
        vmem = pl.BlockSpec(memory_space=pltpu.VMEM)
        hbm = pl.BlockSpec(memory_space=pl.ANY)
        bf16, f32 = jnp.bfloat16, jnp.float32
        scratch = [
            pltpu.VMEM((rows, res_ch), bf16),
            pltpu.VMEM((rows, skip_ch), f32),
            pltpu.VMEM((cycle, res_ch, 2 * gate), bf16),
            pltpu.VMEM((cycle, res_ch, 2 * gate), bf16),
            pltpu.VMEM((cycle, gate, res_ch), bf16),
            pltpu.VMEM((cycle, gate, skip_ch), bf16),
            pltpu.VMEM((sum(halo_rows(k) for k in range(cycle)), res_ch), bf16),
        ]
        scratch += [pltpu.VMEM((stacks, halo_rows(k), res_ch), bf16) for k in range(cycle)]
        scratch += [
            pltpu.SemaphoreType.DMA,
            pltpu.SemaphoreType.DMA((cycle, 4)),
            pltpu.SemaphoreType.DMA((cycle, max_pieces)),
            pltpu.SemaphoreType.DMA((stacks, cycle, max_pieces)),
            pltpu.SemaphoreType.DMA((2,)),
        ]
        macs = rows * (4 * res_ch * gate + gate * (res_ch + skip_ch))
        return pl.pallas_call(
            functools.partial(wavenet_kernel, n_sp, stacks, cycle),
            out_shape=(jax.ShapeDtypeStruct((rows, w_out2.shape[-1]), f32),
                       jax.ShapeDtypeStruct((rows, res_ch), bf16)),
            in_specs=[hbm, hbm, hbm, vmem, hbm, hbm, vmem, vmem, vmem, vmem],
            out_specs=(hbm, hbm),
            scratch_shapes=scratch,
            compiler_params=pltpu.CompilerParams(collective_id=0, has_side_effects=True,
                                                 vmem_limit_bytes=60 * 1024 * 1024),
            cost_estimate=pl.CostEstimate(flops=2 * macs * stacks * cycle, bytes_accessed=90 * 2 ** 20,
                                          transcendentals=0),
            name="wavenet",
        )(x_seq, w_past, w_now, b_conv, w_res, w_skip, w_out1, b_out1.reshape(1, -1), w_out2, b_out2.reshape(1, -1))

    return jax.shard_map(
        local_stack,
        mesh=mesh,
        in_specs=(row_spec, P(), P(), P(), P(), P(), P(), P(), P(), P()),
        out_specs=(row_spec, row_spec),
        check_vma=False,
    )
```

```python
import functools

import jax
import jax.numpy as jnp
from jax import lax
from jax.experimental import pallas as pl
from jax.experimental.pallas import tpu as pltpu
from jax.sharding import PartitionSpec as P

TILE = 16
ROWS = 128
CHUNK = 256
PRE = 32
LOOK = 3
VMEM_MIB = 52
MESH = pl.DeviceIdType.MESH


def halo_rows(k):
    return PRE if k == 0 else 2 ** k if 2 ** k >= PRE else 0


def pieces(rows, k):
    lo, hi, out = rows - halo_rows(k), rows, []
    while hi > lo:
        out.append((max(lo, hi - ROWS), hi))
        hi = max(lo, hi - ROWS)
    return out


def schedule(rows):
    def cut(k, *cuts):
        return [(k, a, b) for a, b in zip(cuts[1:], cuts[:-1])]

    q = rows // 4
    items = []
    for k in range(4):
        items += cut(k, rows, 3 * q, 2 * q, q, -PRE)
    items += cut(4, rows, 3 * q, 2 * q, q, 0)
    items += cut(5, rows, 384, 272, 144, 32)
    items += cut(6, rows, 368, 224, 96)
    items += cut(7, rows, 368)
    items += cut(5, 32, 0)
    items += cut(7, 368, 224)
    items += cut(6, 96, 0)
    items += [("skip", (0, 1, 2, 3), 0, 256), ("skip", (0, 1, 2, 3), 256, 512)]
    items += cut(7, 224, 112, 0)
    items += cut(8, rows, 3 * q, 2 * q)
    items += [("skip", (4, 5, 6, 7), 0, 256), ("skip", (4, 5, 6, 7), 256, 512)]
    items += cut(8, 2 * q, q, 0)
    items += [("skip", (8,), 256, 512)]
    items += cut(9, rows, 3 * q, 2 * q, q, 0)
    items += [("skip", (8,), 0, 256)]
    return items


def wavenet_kernel(n_sp, stacks, cycle, x_ref, wp_ref, wn_ref, b_ref, wr_ref, ws_ref,
                   hbuf, skip, bias_v, gbuf, wp, wn, wr, ws, stage, *scratch):
    halo_layers = [k for k in range(cycle) if halo_rows(k)]
    halos = dict(zip(halo_layers, scratch))
    x_sem, b_sem, w_sem, send_sem, recv_sem = scratch[len(halo_layers):]
    me = lax.axis_index("sp")
    ens = lax.axis_index("ens")
    right = lax.rem(me + 1, n_sp)
    left = lax.rem(me + n_sp - 1, n_sp)
    first = me == 0
    rows = hbuf.shape[0] - PRE
    gate = wr.shape[1]
    f32, bf16 = jnp.float32, jnp.bfloat16
    zero = jnp.zeros((), bf16)

    def weight_copies(stack, k, turn=None):
        par = lax.rem(stack if turn is None else turn, 2)
        return [pltpu.make_async_copy(src.at[stack, k], dst, w_sem.at[k, i])
                for i, (src, dst) in enumerate(((wn_ref, wn.at[k]), (wp_ref, wp.at[k]), (wr_ref, wr.at[k]),
                                                (ws_ref, ws.at[par, k])))]

    stage_off = {}
    off = 0
    for k in halo_layers:
        stage_off[k] = off
        off += halo_rows(k)

    def send(stack, k, p):
        a, b = pieces(rows, k)[p]
        lo = rows - halo_rows(k)
        return pltpu.make_async_remote_copy(
            src_ref=stage.at[pl.ds(stage_off[k] + a - lo, b - a)],
            dst_ref=halos[k].at[stack, pl.ds(a - lo, b - a)],
            send_sem=send_sem.at[k, p],
            recv_sem=recv_sem.at[stack, k, p],
            device_id=(ens, right),
            device_id_type=MESH,
        )

    x_copy = pltpu.make_async_copy(x_ref, hbuf.at[pl.ds(PRE, rows)], x_sem)
    x_copy.start()
    b_copy = pltpu.make_async_copy(b_ref, bias_v, b_sem)
    b_copy.start()
    for c in weight_copies(0, 0):
        c.start()

    barrier = pltpu.get_barrier_semaphore()
    for other in (left, right):
        pl.semaphore_signal(barrier, inc=1, device_id=(ens, other), device_id_type=MESH)
    pl.semaphore_wait(barrier, 2)

    for k in range(1, LOOK):
        for c in weight_copies(0, k):
            c.start()
    skip[...] = jnp.zeros_like(skip)
    x_copy.wait()
    b_copy.wait()

    def load(a, b):
        return hbuf[PRE + a:PRE + b, :]

    def masked(v):
        return jnp.where(first, zero, v)

    def past_rows(stack, k, r0, r1):
        d = 2 ** k
        if d >= rows:
            return masked(halos[k][stack, r0:r1, :])
        a, b = r0 - d, r1 - d
        if d >= TILE:
            if halo_rows(k) == 0:
                return load(a, b)
            parts = []
            if a < 0:
                h = halo_rows(k)
                parts.append(masked(halos[k][stack, h + a:h + min(b, 0), :]))
            if b > 0:
                parts.append(load(max(a, 0), b))
            return parts[0] if len(parts) == 1 else jnp.concatenate(parts, axis=0)
        if r0 == -PRE:
            v = load(r0, r1)
            v = jnp.concatenate([jnp.zeros((TILE, v.shape[1]), bf16), v], axis=0)
        else:
            v = load(r0 - TILE, r1)
        v = v.astype(f32)[TILE - d:TILE - d + r1 - r0]
        return v.astype(bf16)

    def body(stack, carry):
        seen, arrived = set(), set()
        version = {r: 0 for r in range(-PRE, rows, TILE)}
        got = {k: set() for k in range(cycle)}
        sent = set()

        def use_weights(k):
            if k in seen:
                return
            seen.add(k)
            nxt = k + LOOK
            ahead = stack if nxt < cycle else jnp.minimum(stack + 1, stacks - 1)
            for c in weight_copies(ahead, nxt % cycle, stack if nxt < cycle else stack + 1):
                c.start()
            for c in weight_copies(stack, k):
                c.wait()

        def missing(unit):
            k, r0, r1 = unit
            if not halo_rows(k):
                return []
            d = halo_rows(k)
            return [p for p, (a, b) in enumerate(pieces(rows, k))
                    if (k, p) not in arrived and r0 - d < b - rows and min(r1 - d, 0) > a - rows]

        def check(unit):
            k, r0, r1 = unit
            d = 2 ** k
            for r in range(max(r0 - (d if d < rows else 0), -PRE if k < 5 else 0) // TILE * TILE, r1, TILE):
                assert version[r] == k or (r < r0 - TILE and r < 0), (unit, r, version[r])

        def wait_halo(unit):
            k = unit[0]
            for p in missing(unit):
                arrived.add((k, p))
                send(stack, k, p).wait_recv()
                if k == 0:
                    hbuf[0:PRE, :] = masked(halos[0][stack])

        def dots(unit, w, lhs):
            k = unit[0]
            return [[jnp.dot(lhs, w[k, :, b + c * CHUNK:b + (c + 1) * CHUNK], preferred_element_type=f32)
                     for b in (0, gate)] for c in range(gate // CHUNK)]

        def gated(unit, z, c):
            k = unit[0]
            bias = bias_v[k, stack]
            zt = z[0] + bias[None, c * CHUNK:(c + 1) * CHUNK]
            zs = z[1] + bias[None, gate + c * CHUNK:gate + (c + 1) * CHUNK]
            sig = 0.5 * jnp.tanh(0.5 * zs) + 0.5
            return (jnp.tanh(zt) * sig).astype(bf16)

        def finish(unit, g):
            k, r0, r1 = unit
            g = jnp.concatenate(g, axis=1)
            h = load(r0, r1).astype(f32) + jnp.dot(g, wr[k], preferred_element_type=f32)
            h = h.astype(bf16)
            if r0 < 0:
                hbuf[PRE + r0:PRE, :] = masked(h[:-r0])
                hbuf[PRE:PRE + r1, :] = h[-r0:]
                gpos = g[-r0:]
            else:
                hbuf[PRE + r0:PRE + r1, :] = h
                gpos = g
            if k == cycle - 1:
                skip[max(r0, 0):r1, :] += jnp.dot(gpos, ws[lax.rem(stack, 2), k], preferred_element_type=f32)
            else:
                gbuf[k, max(r0, 0):r1, :] = gpos
            for r in range(r0, r1, TILE):
                version[r] = k + 1
                got[k].add(r)
            nk = (k + 1) % cycle
            if not halo_rows(nk):
                return
            lo = rows - halo_rows(nk)
            todo = [(p, a, b) for p, (a, b) in enumerate(pieces(rows, nk))
                    if (nk, p) not in sent and all(r in got[k] for r in range(a, b, TILE))]

            def go():
                s, e = max(r0, lo), r1
                if nk == 0:
                    send(stack, nk, 0).wait_send()
                if s < e:
                    stage[stage_off[nk] + s - lo:stage_off[nk] + e - lo, :] = h[s - r0:e - r0]
                for p, a, b in todo:
                    sent.add((nk, p))
                    send(stack + (1 if nk == 0 else 0), nk, p).start()

            if r1 > lo:
                go()

        def skip_sum(ks, r0, r1):
            acc = jnp.dot(gbuf[ks[0], r0:r1, :], ws[lax.rem(stack, 2), ks[0]], preferred_element_type=f32)
            for k in ks[1:]:
                acc = acc + jnp.dot(gbuf[k, r0:r1, :], ws[lax.rem(stack, 2), k], preferred_element_type=f32)
            skip[r0:r1, :] += acc

        chunks = range(gate // CHUNK)
        prev = None

        def flush():
            nonlocal prev
            if prev is not None:
                unit, z = prev
                prev = None
                finish(unit, [gated(unit, z[c], c) for c in chunks])

        plan = schedule(rows)
        for n, item in enumerate(plan):
            if item[0] == "skip":
                skip_sum(*item[1:])
                continue
            k, r0, r1 = item
            use_weights(k)
            for later in plan[n + 1:n + 2]:
                if later[0] != "skip":
                    use_weights(later[0])
            if prev is not None:
                (pk, p0, p1), d = prev[0], 2 ** k
                if pk == k - 1 and max(r0 - (d if d < rows else 0), -PRE) < p1 and p0 < r1:
                    flush()
            if missing(item):
                if k == 0:
                    flush()
                    wait_halo(item)
                    check(item)
                    zn = dots(item, wn, load(r0, r1))
                else:
                    zn = dots(item, wn, load(r0, r1))
                    flush()
                    wait_halo(item)
                    check(item)
                zp = dots(item, wp, past_rows(stack, k, r0, r1))
                z = [[zp[c][i] + zn[c][i] for i in range(2)] for c in chunks]
                flush()
            else:
                check(item)
                past, now = past_rows(stack, k, r0, r1), load(r0, r1)
                zp, zn = dots(item, wp, past), dots(item, wn, now)
                z = [[zp[c][i] + zn[c][i] for i in range(2)] for c in chunks]
                flush()
            prev = (item, z)
        flush()
        for k in halo_layers[1:]:
            for p in range(len(pieces(rows, k))):
                send(stack, k, p).wait_send()
        return carry

    stage[0:PRE, :] = load(rows - PRE, rows)
    send(0, 0, 0).start()
    lax.fori_loop(0, stacks, body, 0)
    send(stacks, 0, 0).wait()
    for k in range(LOOK):
        for c in weight_copies(stacks - 1, k, stacks):
            c.wait()


def head_kernel(hbuf, skip, w1_ref, c1_ref, w2_ref, c2_ref, y_ref, hout_ref, logits, sems):
    f32, bf16 = jnp.float32, jnp.bfloat16
    rows = skip.shape[0]
    h_copy = pltpu.make_async_copy(hbuf.at[pl.ds(PRE, rows)], hout_ref, sems.at[0])
    h_copy.start()
    a = jnp.maximum(skip[...], 0.0).astype(bf16)
    m = jnp.dot(a, w1_ref[...], preferred_element_type=f32) + c1_ref[...]
    m = jnp.maximum(m, 0.0).astype(bf16)
    logits[...] = jnp.dot(m, w2_ref[...], preferred_element_type=f32) + c2_ref[...]
    y_copy = pltpu.make_async_copy(logits, y_ref, sems.at[1])
    y_copy.start()
    h_copy.wait()
    y_copy.wait()


def solution(mesh):
    n_sp = mesh.shape["sp"]
    row_spec = P(("ens", "sp"), None)

    def local_stack(x_seq, w_past, w_now, b_conv, w_res, w_skip, w_out1, b_out1, w_out2, b_out2):
        rows, res_ch = x_seq.shape
        stacks, cycle = w_past.shape[:2]
        skip_ch = w_skip.shape[-1]
        gate = w_res.shape[2]
        max_pieces = max(1, 2 ** (cycle - 1) // ROWS)
        vmem = pl.BlockSpec(memory_space=pltpu.VMEM)
        hbm = pl.BlockSpec(memory_space=pltpu.HBM)
        bf16, f32 = jnp.bfloat16, jnp.float32
        scratch = [
            pltpu.VMEM((cycle, stacks, 2 * gate), f32),
            pltpu.VMEM((cycle - 1, rows, gate), bf16),
            pltpu.VMEM((cycle, res_ch, 2 * gate), bf16),
            pltpu.VMEM((cycle, res_ch, 2 * gate), bf16),
            pltpu.VMEM((cycle, gate, res_ch), bf16),
            pltpu.VMEM((2, cycle, gate, skip_ch), bf16),
            pltpu.VMEM((sum(halo_rows(k) for k in range(cycle)), res_ch), bf16),
        ]
        scratch += [pltpu.VMEM((stacks + (k == 0), halo_rows(k), res_ch), bf16) for k in range(cycle) if halo_rows(k)]
        scratch += [
            pltpu.SemaphoreType.DMA,
            pltpu.SemaphoreType.DMA,
            pltpu.SemaphoreType.DMA((cycle, 4)),
            pltpu.SemaphoreType.DMA((cycle, max_pieces)),
            pltpu.SemaphoreType.DMA((stacks + 1, cycle, max_pieces)),
        ]
        macs = rows * (4 * res_ch * gate + gate * (res_ch + skip_ch))
        hidden, skip = pl.pallas_call(
            functools.partial(wavenet_kernel, n_sp, stacks, cycle),
            out_shape=(jax.ShapeDtypeStruct((PRE + rows, res_ch), bf16),
                       jax.ShapeDtypeStruct((rows, skip_ch), f32)),
            in_specs=[hbm] * 6,
            out_specs=(vmem, vmem),
            scratch_shapes=scratch,
            compiler_params=pltpu.CompilerParams(collective_id=0, has_side_effects=True,
                                                 vmem_limit_bytes=VMEM_MIB * 2 ** 20),
            cost_estimate=pl.CostEstimate(flops=2 * macs * stacks * cycle, bytes_accessed=90 * 2 ** 20,
                                          transcendentals=0),
            name="wavenet",
        )(x_seq, w_past, w_now, jnp.transpose(b_conv, (1, 0, 2)), w_res, w_skip)
        return pl.pallas_call(
            head_kernel,
            out_shape=(jax.ShapeDtypeStruct((rows, w_out2.shape[-1]), f32),
                       jax.ShapeDtypeStruct((rows, res_ch), bf16)),
            in_specs=[vmem] * 6,
            out_specs=(hbm, hbm),
            scratch_shapes=[pltpu.VMEM((rows, w_out2.shape[-1]), f32), pltpu.SemaphoreType.DMA((2,))],
            compiler_params=pltpu.CompilerParams(vmem_limit_bytes=8 * 2 ** 20),
            name="head",
        )(hidden, skip, w_out1, b_out1.reshape(1, -1), w_out2, b_out2.reshape(1, -1))

    return jax.shard_map(
        local_stack,
        mesh=mesh,
        in_specs=(row_spec, P(), P(), P(), P(), P(), P(), P(), P(), P()),
        out_specs=(row_spec, row_spec),
        check_vma=False,
    )
```

```python
import functools

import jax
import jax.numpy as jnp
from jax import lax
from jax.experimental import pallas as pl
from jax.experimental.pallas import tpu as pltpu
from jax.sharding import PartitionSpec as P

TILE = 16
ROWS = 128
CHUNK = 256
PRE = 32
LATE = (7, 8, 9)
LOOK = 3
VMEM_MIB = 58
MESH = pl.DeviceIdType.MESH


def halo_rows(k):
    return PRE if k == 0 else 2 ** k if 2 ** k >= PRE else 0


def pieces(rows, k):
    lo, hi, out = rows - halo_rows(k), rows, []
    while hi > lo:
        out.append((max(lo, hi - ROWS), hi))
        hi = max(lo, hi - ROWS)
    return out


def schedule(rows):
    def cut(k, *cuts):
        return [(k, a, b) for a, b in zip(cuts[1:], cuts[:-1])]

    q = rows // 4
    items = []
    for k in range(4):
        items += cut(k, rows, 3 * q, 2 * q, q, -PRE)
    items += cut(4, rows, 3 * q, 2 * q, q, 0)
    items += cut(5, rows, 384, 272, 144, 32)
    items += cut(6, rows, 368, 224, 96)
    items += cut(7, rows, 368)
    items += cut(5, 32, 0)
    items += cut(7, 368, 224)
    items += cut(6, 96, 0)
    items += cut(7, 224, 112, 0)
    items += cut(8, rows, 3 * q, 2 * q)
    items += [("skip", (0, 1, 2, 3), 0, 256), ("skip", (0, 1, 2, 3), 256, 512)]
    items += cut(8, 2 * q, q, 0)
    items += [("skip", (4, 5, 6, 7, 8), 256, 512), ("skip", (4, 5, 6, 7), 0, 256)]
    items += cut(9, rows, 3 * q)
    items += [("skip", (8,), 0, 256)]
    items += cut(9, 3 * q, 2 * q, q, 0)
    return items


def wavenet_kernel(n_sp, stacks, cycle, x_ref, wp_ref, wn_ref, b_ref, wr_ref, ws_ref,
                   hbuf, skip, bias_v, gbuf, wp, wn, wr, ws, stage, *scratch):
    halo_layers = [k for k in range(cycle) if halo_rows(k)]
    halos = dict(zip(halo_layers, scratch))
    x_sem, b_sem, w_sem, send_sem, recv_sem = scratch[len(halo_layers):]
    me = lax.axis_index("sp")
    ens = lax.axis_index("ens")
    last = lax.div(me, n_sp - 1)
    target = me + 1 - 2 * last
    spare = stacks + 1
    first = me == 0
    rows = hbuf.shape[0] - PRE
    gate = wr.shape[1]
    f32, bf16 = jnp.float32, jnp.bfloat16
    zero = jnp.zeros((), bf16)

    def weight_copies(stack, k, turn=None):
        par = lax.rem(stack if turn is None else turn, 2)
        return [pltpu.make_async_copy(src.at[stack, k], dst, w_sem.at[k, i])
                for i, (src, dst) in enumerate(((wn_ref, wn.at[k]), (wp_ref, wp.at[k]), (wr_ref, wr.at[k]),
                                                (ws_ref, ws.at[par, k])))]

    stage_off = {}
    off = 0
    for k in halo_layers:
        stage_off[k] = off
        off += halo_rows(k)

    def send(stack, k, p):
        a, b = pieces(rows, k)[p]
        lo = rows - halo_rows(k)
        return pltpu.make_async_remote_copy(
            src_ref=stage.at[stack, pl.ds(stage_off[k] + a - lo, b - a)],
            dst_ref=halos[k].at[stack + spare * last, pl.ds(a - lo, b - a)],
            send_sem=send_sem.at[stack, k, p],
            recv_sem=recv_sem.at[stack + spare * last, k, p],
            device_id=(ens, target),
            device_id_type=MESH,
        )

    def arrival(slot, k, p):
        a, b = pieces(rows, k)[p]
        lo = rows - halo_rows(k)
        return pltpu.make_async_copy(x_ref.at[pl.ds(a - lo, b - a)], halos[k].at[slot, pl.ds(a - lo, b - a)],
                                     recv_sem.at[slot, k, p])

    every = [(slot, k, p) for slot in range(stacks + 1) for k in halo_layers if slot < stacks or k == 0
             for p in range(len(pieces(rows, k)))]
    x_copy = pltpu.make_async_copy(x_ref, hbuf.at[pl.ds(PRE, rows)], x_sem)
    x_copy.start()
    b_copy = pltpu.make_async_copy(b_ref, bias_v, b_sem)
    b_copy.start()
    for c in weight_copies(0, 0):
        c.start()

    barrier = pltpu.get_barrier_semaphore()

    @pl.when(me > 0)
    def _():
        pl.semaphore_signal(barrier, inc=1, device_id=(ens, me - 1), device_id_type=MESH)

    @pl.when(me == n_sp - 2)
    def _():
        pl.semaphore_signal(barrier, inc=1, device_id=(ens, me + 1), device_id_type=MESH)

    pl.semaphore_wait(barrier, 1)

    for k in range(1, LOOK):
        for c in weight_copies(0, k):
            c.start()
    @pl.when(me == 0)
    def _():
        for t in every:
            arrival(*t).start()

    skip[...] = jnp.zeros_like(skip)
    x_copy.wait()
    b_copy.wait()

    def load(a, b):
        return hbuf[PRE + a:PRE + b, :]

    def masked(v):
        return jnp.where(first, zero, v)

    def past_rows(stack, k, r0, r1):
        d = 2 ** k
        if d >= rows:
            return masked(halos[k][stack, r0:r1, :])
        a, b = r0 - d, r1 - d
        if d >= TILE:
            if halo_rows(k) == 0:
                return load(a, b)
            parts = []
            if a < 0:
                h = halo_rows(k)
                parts.append(masked(halos[k][stack, h + a:h + min(b, 0), :]))
            if b > 0:
                parts.append(load(max(a, 0), b))
            return parts[0] if len(parts) == 1 else jnp.concatenate(parts, axis=0)
        if r0 == -PRE:
            v = load(r0, r1)
            v = jnp.concatenate([jnp.zeros((TILE, v.shape[1]), bf16), v], axis=0)
        else:
            v = load(r0 - TILE, r1)
        v = v.astype(f32)[TILE - d:TILE - d + r1 - r0]
        return v.astype(bf16)

    def body(stack, carry):
        seen, arrived = set(), set()
        version = {r: 0 for r in range(-PRE, rows, TILE)}
        got = {k: set() for k in range(cycle)}
        sent = set()
        ready = []

        def use_weights(k):
            if k in seen:
                return
            seen.add(k)
            nxt = k + LOOK
            ahead = stack if nxt < cycle else jnp.minimum(stack + 1, stacks - 1)
            for c in weight_copies(ahead, nxt % cycle, stack if nxt < cycle else stack + 1):
                c.start()
            for c in weight_copies(stack, k):
                c.wait()

        def missing(unit):
            k, r0, r1 = unit
            if not halo_rows(k):
                return []
            d = halo_rows(k)
            return [p for p, (a, b) in enumerate(pieces(rows, k))
                    if (k, p) not in arrived and r0 - d < b - rows and min(r1 - d, 0) > a - rows]

        def check(unit):
            k, r0, r1 = unit
            d = 2 ** k
            for r in range(max(r0 - (d if d < rows else 0), -PRE if k < 5 else 0) // TILE * TILE, r1, TILE):
                assert version[r] == k or (r < r0 - TILE and r < 0), (unit, r, version[r])

        def wait_halo(unit):
            k = unit[0]
            for p in missing(unit):
                arrived.add((k, p))
                arrival(stack, k, p).wait()
                if k == 0:
                    hbuf[0:PRE, :] = masked(halos[0][stack])

        def dots(unit, w, lhs):
            k = unit[0]
            return [[jnp.dot(lhs, w[k, :, b + c * CHUNK:b + (c + 1) * CHUNK], preferred_element_type=f32)
                     for b in (0, gate)] for c in range(gate // CHUNK)]

        def gated(unit, z, c):
            k = unit[0]
            bias = bias_v[k, stack]
            zt = z[0] + bias[None, c * CHUNK:(c + 1) * CHUNK]
            zs = z[1] + bias[None, gate + c * CHUNK:gate + (c + 1) * CHUNK]
            sig = 0.5 * jnp.tanh(0.5 * zs) + 0.5
            return (jnp.tanh(zt) * sig).astype(bf16)

        def finish(unit, g):
            k, r0, r1 = unit
            g = jnp.concatenate(g, axis=1)
            h = load(r0, r1).astype(f32) + jnp.dot(g, wr[k], preferred_element_type=f32)
            h = h.astype(bf16)
            if r0 < 0:
                hbuf[PRE + r0:PRE, :] = masked(h[:-r0])
                hbuf[PRE:PRE + r1, :] = h[-r0:]
                gpos = g[-r0:]
            else:
                hbuf[PRE + r0:PRE + r1, :] = h
                gpos = g
            if k == cycle - 1:
                skip[max(r0, 0):r1, :] += jnp.dot(gpos, ws[lax.rem(stack, 2), k], preferred_element_type=f32)
            else:
                gbuf[k, max(r0, 0):r1, :] = gpos
            for r in range(r0, r1, TILE):
                version[r] = k + 1
                got[k].add(r)
            nk = (k + 1) % cycle
            if not halo_rows(nk):
                return
            lo = rows - halo_rows(nk)
            todo = [(p, a, b) for p, (a, b) in enumerate(pieces(rows, nk))
                    if (nk, p) not in sent and all(r in got[k] for r in range(a, b, TILE))]

            def go():
                s, e = max(r0, lo), r1
                if s < e:
                    stage[stack + (nk == 0), stage_off[nk] + s - lo:stage_off[nk] + e - lo, :] = h[s - r0:e - r0]
                for p, a, b in todo:
                    sent.add((nk, p))
                    ready.append((stack + (1 if nk == 0 else 0), nk, p))

            if r1 > lo:
                go()

        def skip_sum(ks, r0, r1):
            assert all(r in got[k] for k in ks for r in range(r0, r1, TILE)), (ks, r0, r1)
            acc = jnp.dot(gbuf[ks[0], r0:r1, :], ws[lax.rem(stack, 2), ks[0]], preferred_element_type=f32)
            for k in ks[1:]:
                acc = acc + jnp.dot(gbuf[k, r0:r1, :], ws[lax.rem(stack, 2), k], preferred_element_type=f32)
            skip[r0:r1, :] += acc

        chunks = range(gate // CHUNK)
        prev = None

        def start_sends():
            for t in ready:
                send(*t).start()
            ready.clear()

        def flush():
            nonlocal prev
            if prev is not None:
                unit, z = prev
                prev = None
                finish(unit, [gated(unit, z[c], c) for c in chunks])

        plan = schedule(rows)
        for n, item in enumerate(plan):
            if item[0] == "skip":
                skip_sum(*item[1:])
                start_sends()
                continue
            k, r0, r1 = item
            use_weights(k)
            for later in plan[n + 1:n + 2]:
                if later[0] != "skip":
                    use_weights(later[0])
            if prev is not None:
                (pk, p0, p1), d = prev[0], 2 ** k
                if pk == k - 1 and max(r0 - (d if d < rows else 0), -PRE) < p1 and p0 < r1:
                    flush()
            late = k in LATE and missing(item)
            if k == 0:
                wait_halo(item)
            zn = dots(item, wn, load(r0, r1))
            if late:
                flush()
            start_sends()
            wait_halo(item)
            check(item)
            zp = dots(item, wp, past_rows(stack, k, r0, r1))
            z = [[zp[c][i] + zn[c][i] for i in range(2)] for c in chunks]
            flush()
            prev = (item, z)
        flush()
        start_sends()
        return carry

    stage[0, 0:PRE, :] = load(rows - PRE, rows)
    send(0, 0, 0).start()
    lax.fori_loop(0, stacks, body, 0)
    for t in every:
        send(*t).wait_send()
    arrival(stacks, 0, 0).wait()

    @pl.when(me == n_sp - 2)
    def _():
        for slot, k, p in every:
            arrival(slot + spare, k, p).wait()

    for k in range(LOOK):
        for c in weight_copies(stacks - 1, k, stacks):
            c.wait()


def head_kernel(hbuf, skip, w1_ref, c1_ref, w2_ref, c2_ref, y_ref, hout_ref, logits, sems):
    f32, bf16 = jnp.float32, jnp.bfloat16
    rows = skip.shape[0]
    h_copy = pltpu.make_async_copy(hbuf.at[pl.ds(PRE, rows)], hout_ref, sems.at[0])
    h_copy.start()
    a = jnp.maximum(skip[...], 0.0).astype(bf16)
    m = jnp.dot(a, w1_ref[...], preferred_element_type=f32) + c1_ref[...]
    m = jnp.maximum(m, 0.0).astype(bf16)
    logits[...] = jnp.dot(m, w2_ref[...], preferred_element_type=f32) + c2_ref[...]
    y_copy = pltpu.make_async_copy(logits, y_ref, sems.at[1])
    y_copy.start()
    h_copy.wait()
    y_copy.wait()


def solution(mesh):
    n_sp = mesh.shape["sp"]
    row_spec = P(("ens", "sp"), None)

    def local_stack(x_seq, w_past, w_now, b_conv, w_res, w_skip, w_out1, b_out1, w_out2, b_out2):
        rows, res_ch = x_seq.shape
        stacks, cycle = w_past.shape[:2]
        skip_ch = w_skip.shape[-1]
        gate = w_res.shape[2]
        max_pieces = max(1, 2 ** (cycle - 1) // ROWS)
        vmem = pl.BlockSpec(memory_space=pltpu.VMEM)
        hbm = pl.BlockSpec(memory_space=pltpu.HBM)
        bf16, f32 = jnp.bfloat16, jnp.float32
        scratch = [
            pltpu.VMEM((cycle, stacks, 2 * gate), f32),
            pltpu.VMEM((cycle - 1, rows, gate), bf16),
            pltpu.VMEM((cycle, res_ch, 2 * gate), bf16),
            pltpu.VMEM((cycle, res_ch, 2 * gate), bf16),
            pltpu.VMEM((cycle, gate, res_ch), bf16),
            pltpu.VMEM((2, cycle, gate, skip_ch), bf16),
            pltpu.VMEM((stacks + 1, sum(halo_rows(k) for k in range(cycle)), res_ch), bf16),
        ]
        scratch += [pltpu.VMEM((2 * (stacks + 1), halo_rows(k), res_ch), bf16) for k in range(cycle) if halo_rows(k)]
        scratch += [
            pltpu.SemaphoreType.DMA,
            pltpu.SemaphoreType.DMA,
            pltpu.SemaphoreType.DMA((cycle, 4)),
            pltpu.SemaphoreType.DMA((stacks + 1, cycle, max_pieces)),
            pltpu.SemaphoreType.DMA((2 * (stacks + 1), cycle, max_pieces)),
        ]
        macs = rows * (4 * res_ch * gate + gate * (res_ch + skip_ch))
        hidden, skip = pl.pallas_call(
            functools.partial(wavenet_kernel, n_sp, stacks, cycle),
            out_shape=(pltpu.VMEM((PRE + rows, res_ch), bf16), pltpu.VMEM((rows, skip_ch), f32)),
            in_specs=[hbm] * 6,
            out_specs=(vmem, vmem),
            scratch_shapes=scratch,
            compiler_params=pltpu.CompilerParams(collective_id=0, has_side_effects=True,
                                                 vmem_limit_bytes=VMEM_MIB * 2 ** 20),
            cost_estimate=pl.CostEstimate(flops=2 * macs * stacks * cycle, bytes_accessed=90 * 2 ** 20,
                                          transcendentals=0),
            name="wavenet",
        )(x_seq, w_past, w_now, jnp.transpose(b_conv, (1, 0, 2)), w_res, w_skip)
        return pl.pallas_call(
            head_kernel,
            out_shape=(jax.ShapeDtypeStruct((rows, w_out2.shape[-1]), f32),
                       jax.ShapeDtypeStruct((rows, res_ch), bf16)),
            in_specs=[vmem] * 6,
            out_specs=(hbm, hbm),
            scratch_shapes=[pltpu.VMEM((rows, w_out2.shape[-1]), f32), pltpu.SemaphoreType.DMA((2,))],
            compiler_params=pltpu.CompilerParams(vmem_limit_bytes=8 * 2 ** 20),
            name="head",
        )(hidden, skip, w_out1, b_out1.reshape(1, -1), w_out2, b_out2.reshape(1, -1))

    return jax.shard_map(
        local_stack,
        mesh=mesh,
        in_specs=(row_spec, P(), P(), P(), P(), P(), P(), P(), P(), P()),
        out_specs=(row_spec, row_spec),
        check_vma=False,
    )
```

```python
import functools

import jax
import jax.numpy as jnp
from jax import lax
from jax.experimental import pallas as pl
from jax.experimental.pallas import tpu as pltpu
from jax.sharding import PartitionSpec as P

TILE = 16
ROWS = 128
CHUNK = 256
PRE = 32
LATE = (8, 9)
LOOK = 3
VMEM_MIB = 58
MESH = pl.DeviceIdType.MESH


def halo_rows(k):
    return PRE if k == 0 else 2 ** k if 2 ** k >= PRE else 0


def pieces(rows, k):
    lo, hi, out = rows - halo_rows(k), rows, []
    while hi > lo:
        out.append((max(lo, hi - ROWS), hi))
        hi = max(lo, hi - ROWS)
    return out


def schedule(rows):
    def cut(k, *cuts):
        return [(k, a, b) for a, b in zip(cuts[1:], cuts[:-1])]

    q = rows // 4
    items = []
    for k in range(4):
        items += cut(k, rows, 3 * q, 2 * q, q, -PRE)
    items += cut(4, rows, 3 * q, 2 * q, q, 0)
    items += cut(5, rows, 384, 272, 144, 32)
    items += cut(6, rows, 368, 224, 96)
    items += cut(7, rows, 368)
    items += cut(5, 32, 0)
    items += cut(7, 368, 224)
    items += cut(6, 96, 0)
    items += cut(7, 224, 112, 0)
    items += cut(8, rows, 3 * q, 2 * q)
    items += [("skip", (0, 1, 2, 3), 256, 512)]
    items += cut(8, 2 * q, q, 0)
    items += [("skip", (4, 5, 6, 7, 8), 256, 512), ("skip", (4, 5, 6, 7), 0, 256)]
    items += cut(9, rows, 3 * q)
    items += [("skip", (0, 1, 2, 3, 8), 0, 256)]
    items += cut(9, 3 * q, 2 * q, q, 0)
    return items


def wavenet_kernel(n_sp, stacks, cycle, x_ref, wp_ref, wn_ref, b_ref, wr_ref, ws_ref,
                   hbuf, skip, bias_v, gbuf, wp, wn, wr, ws, stage, *scratch):
    halo_layers = [k for k in range(cycle) if halo_rows(k)]
    halos = dict(zip(halo_layers, scratch))
    x_sem, b_sem, w_sem, send_sem, recv_sem = scratch[len(halo_layers):]
    me = lax.axis_index("sp")
    ens = lax.axis_index("ens")
    last = lax.div(me, n_sp - 1)
    target = me + 1 - 2 * last
    spare = stacks + 1
    first = me == 0
    rows = hbuf.shape[0] - PRE
    gate = wr.shape[1]
    f32, bf16 = jnp.float32, jnp.bfloat16
    zero = jnp.zeros((), bf16)

    def weight_copies(stack, k, turn=None):
        par = lax.rem(stack if turn is None else turn, 2)
        return [pltpu.make_async_copy(src.at[stack, k], dst, w_sem.at[k, i])
                for i, (src, dst) in enumerate(((wn_ref, wn.at[k]), (wp_ref, wp.at[k]), (wr_ref, wr.at[k]),
                                                (ws_ref, ws.at[par, k])))]

    stage_off = {}
    off = 0
    for k in halo_layers:
        stage_off[k] = off
        off += halo_rows(k)

    def send(stack, k, p):
        a, b = pieces(rows, k)[p]
        lo = rows - halo_rows(k)
        return pltpu.make_async_remote_copy(
            src_ref=stage.at[stack, pl.ds(stage_off[k] + a - lo, b - a)],
            dst_ref=halos[k].at[stack + spare * last, pl.ds(a - lo, b - a)],
            send_sem=send_sem.at[stack, k, p],
            recv_sem=recv_sem.at[stack + spare * last, k, p],
            device_id=(ens, target),
            device_id_type=MESH,
        )

    def arrival(slot, k, p):
        a, b = pieces(rows, k)[p]
        lo = rows - halo_rows(k)
        return pltpu.make_async_copy(x_ref.at[pl.ds(a - lo, b - a)], halos[k].at[slot, pl.ds(a - lo, b - a)],
                                     recv_sem.at[slot, k, p])

    every = [(slot, k, p) for slot in range(stacks + 1) for k in halo_layers if slot < stacks or k == 0
             for p in range(len(pieces(rows, k)))]
    x_copy = pltpu.make_async_copy(x_ref, hbuf.at[pl.ds(PRE, rows)], x_sem)
    x_copy.start()
    b_copy = pltpu.make_async_copy(b_ref, bias_v, b_sem)
    b_copy.start()
    for c in weight_copies(0, 0):
        c.start()

    barrier = pltpu.get_barrier_semaphore()

    @pl.when(me > 0)
    def _():
        pl.semaphore_signal(barrier, inc=1, device_id=(ens, me - 1), device_id_type=MESH)

    @pl.when(me == n_sp - 2)
    def _():
        pl.semaphore_signal(barrier, inc=1, device_id=(ens, me + 1), device_id_type=MESH)

    pl.semaphore_wait(barrier, 1)

    for k in range(1, LOOK):
        for c in weight_copies(0, k):
            c.start()
    @pl.when(me == 0)
    def _():
        for t in every:
            arrival(*t).start()

    skip[...] = jnp.zeros_like(skip)
    x_copy.wait()
    b_copy.wait()

    def load(a, b):
        return hbuf[PRE + a:PRE + b, :]

    def masked(v):
        return jnp.where(first, zero, v)

    def past_rows(stack, k, r0, r1):
        d = 2 ** k
        if d >= rows:
            return masked(halos[k][stack, r0:r1, :])
        a, b = r0 - d, r1 - d
        if d >= TILE:
            if halo_rows(k) == 0:
                return load(a, b)
            parts = []
            if a < 0:
                h = halo_rows(k)
                parts.append(masked(halos[k][stack, h + a:h + min(b, 0), :]))
            if b > 0:
                parts.append(load(max(a, 0), b))
            return parts[0] if len(parts) == 1 else jnp.concatenate(parts, axis=0)
        if r0 == -PRE:
            v = load(r0, r1)
            v = jnp.concatenate([jnp.zeros((TILE, v.shape[1]), bf16), v], axis=0)
        else:
            v = load(r0 - TILE, r1)
        v = v.astype(f32)[TILE - d:TILE - d + r1 - r0]
        return v.astype(bf16)

    def body(stack, carry):
        seen, arrived = set(), set()
        version = {r: 0 for r in range(-PRE, rows, TILE)}
        got = {k: set() for k in range(cycle)}
        sent = set()
        ready = []

        def use_weights(k):
            if k in seen:
                return
            seen.add(k)
            nxt = k + LOOK
            ahead = stack if nxt < cycle else jnp.minimum(stack + 1, stacks - 1)
            for c in weight_copies(ahead, nxt % cycle, stack if nxt < cycle else stack + 1):
                c.start()
            for c in weight_copies(stack, k):
                c.wait()

        def missing(unit):
            k, r0, r1 = unit
            if not halo_rows(k):
                return []
            d = halo_rows(k)
            return [p for p, (a, b) in enumerate(pieces(rows, k))
                    if (k, p) not in arrived and r0 - d < b - rows and min(r1 - d, 0) > a - rows]

        def check(unit):
            k, r0, r1 = unit
            d = 2 ** k
            for r in range(max(r0 - (d if d < rows else 0), -PRE if k < 5 else 0) // TILE * TILE, r1, TILE):
                assert version[r] == k or (r < r0 - TILE and r < 0), (unit, r, version[r])

        def wait_halo(unit):
            k = unit[0]
            for p in missing(unit):
                arrived.add((k, p))
                arrival(stack, k, p).wait()
                if k == 0:
                    hbuf[0:PRE, :] = masked(halos[0][stack])

        def dots(unit, w, lhs):
            k = unit[0]
            return [[jnp.dot(lhs, w[k, :, b + c * CHUNK:b + (c + 1) * CHUNK], preferred_element_type=f32)
                     for b in (0, gate)] for c in range(gate // CHUNK)]

        def gated(unit, z, c):
            k = unit[0]
            bias = bias_v[k, stack]
            zt = z[0] + bias[None, c * CHUNK:(c + 1) * CHUNK]
            zs = z[1] + bias[None, gate + c * CHUNK:gate + (c + 1) * CHUNK]
            sig = 0.5 * jnp.tanh(0.5 * zs) + 0.5
            return (jnp.tanh(zt) * sig).astype(bf16)

        def finish(unit, g):
            k, r0, r1 = unit
            g = jnp.concatenate(g, axis=1)
            h = load(r0, r1).astype(f32) + jnp.dot(g, wr[k], preferred_element_type=f32)
            h = h.astype(bf16)
            if r0 < 0:
                hbuf[PRE + r0:PRE, :] = masked(h[:-r0])
                hbuf[PRE:PRE + r1, :] = h[-r0:]
                gpos = g[-r0:]
            else:
                hbuf[PRE + r0:PRE + r1, :] = h
                gpos = g
            if k == cycle - 1:
                skip[max(r0, 0):r1, :] += jnp.dot(gpos, ws[lax.rem(stack, 2), k], preferred_element_type=f32)
            else:
                gbuf[k, max(r0, 0):r1, :] = gpos
            for r in range(r0, r1, TILE):
                version[r] = k + 1
                got[k].add(r)
            nk = (k + 1) % cycle
            if not halo_rows(nk):
                return
            lo = rows - halo_rows(nk)
            todo = [(p, a, b) for p, (a, b) in enumerate(pieces(rows, nk))
                    if (nk, p) not in sent and all(r in got[k] for r in range(a, b, TILE))]

            def go():
                s, e = max(r0, lo), r1
                if s < e:
                    stage[stack + (nk == 0), stage_off[nk] + s - lo:stage_off[nk] + e - lo, :] = h[s - r0:e - r0]
                for p, a, b in todo:
                    sent.add((nk, p))
                    ready.append((stack + (1 if nk == 0 else 0), nk, p))

            if r1 > lo:
                go()

        def skip_sum(ks, r0, r1):
            assert all(r in got[k] for k in ks for r in range(r0, r1, TILE)), (ks, r0, r1)
            acc = jnp.dot(gbuf[ks[0], r0:r1, :], ws[lax.rem(stack, 2), ks[0]], preferred_element_type=f32)
            for k in ks[1:]:
                acc = acc + jnp.dot(gbuf[k, r0:r1, :], ws[lax.rem(stack, 2), k], preferred_element_type=f32)
            skip[r0:r1, :] += acc

        chunks = range(gate // CHUNK)
        prev = None

        def start_sends():
            for t in ready:
                send(*t).start()
            ready.clear()

        def flush():
            nonlocal prev
            if prev is not None:
                unit, z = prev
                prev = None
                finish(unit, [gated(unit, z[c], c) for c in chunks])

        plan = schedule(rows)
        for n, item in enumerate(plan):
            if item[0] == "skip":
                skip_sum(*item[1:])
                start_sends()
                continue
            k, r0, r1 = item
            use_weights(k)
            for later in plan[n + 1:n + 2]:
                if later[0] != "skip":
                    use_weights(later[0])
            if prev is not None:
                (pk, p0, p1), d = prev[0], 2 ** k
                if pk == k - 1 and max(r0 - (d if d < rows else 0), -PRE) < p1 and p0 < r1:
                    flush()
            late = k in LATE and missing(item)
            if k == 0:
                wait_halo(item)
            zn = dots(item, wn, load(r0, r1))
            if late:
                flush()
            start_sends()
            wait_halo(item)
            check(item)
            zp = dots(item, wp, past_rows(stack, k, r0, r1))
            z = [[zp[c][i] + zn[c][i] for i in range(2)] for c in chunks]
            flush()
            prev = (item, z)
        flush()
        start_sends()
        return carry

    stage[0, 0:PRE, :] = load(rows - PRE, rows)
    send(0, 0, 0).start()
    lax.fori_loop(0, stacks, body, 0)
    for t in every:
        send(*t).wait_send()
    arrival(stacks, 0, 0).wait()

    @pl.when(me == n_sp - 2)
    def _():
        for slot, k, p in every:
            arrival(slot + spare, k, p).wait()

    for k in range(LOOK):
        for c in weight_copies(stacks - 1, k, stacks):
            c.wait()


def head_kernel(hbuf, skip, w1_ref, c1_ref, w2_ref, c2_ref, y_ref, hout_ref, logits, sems):
    f32, bf16 = jnp.float32, jnp.bfloat16
    rows = skip.shape[0]
    h_copy = pltpu.make_async_copy(hbuf.at[pl.ds(PRE, rows)], hout_ref, sems.at[0])
    h_copy.start()
    a = jnp.maximum(skip[...], 0.0).astype(bf16)
    m = jnp.dot(a, w1_ref[...], preferred_element_type=f32) + c1_ref[...]
    m = jnp.maximum(m, 0.0).astype(bf16)
    logits[...] = jnp.dot(m, w2_ref[...], preferred_element_type=f32) + c2_ref[...]
    y_copy = pltpu.make_async_copy(logits, y_ref, sems.at[1])
    y_copy.start()
    h_copy.wait()
    y_copy.wait()


def solution(mesh):
    n_sp = mesh.shape["sp"]
    row_spec = P(("ens", "sp"), None)

    def local_stack(x_seq, w_past, w_now, b_conv, w_res, w_skip, w_out1, b_out1, w_out2, b_out2):
        rows, res_ch = x_seq.shape
        stacks, cycle = w_past.shape[:2]
        skip_ch = w_skip.shape[-1]
        gate = w_res.shape[2]
        max_pieces = max(1, 2 ** (cycle - 1) // ROWS)
        vmem = pl.BlockSpec(memory_space=pltpu.VMEM)
        hbm = pl.BlockSpec(memory_space=pltpu.HBM)
        bf16, f32 = jnp.bfloat16, jnp.float32
        scratch = [
            pltpu.VMEM((cycle, stacks, 2 * gate), f32),
            pltpu.VMEM((cycle - 1, rows, gate), bf16),
            pltpu.VMEM((cycle, res_ch, 2 * gate), bf16),
            pltpu.VMEM((cycle, res_ch, 2 * gate), bf16),
            pltpu.VMEM((cycle, gate, res_ch), bf16),
            pltpu.VMEM((2, cycle, gate, skip_ch), bf16),
            pltpu.VMEM((stacks + 1, sum(halo_rows(k) for k in range(cycle)), res_ch), bf16),
        ]
        scratch += [pltpu.VMEM((2 * (stacks + 1), halo_rows(k), res_ch), bf16) for k in range(cycle) if halo_rows(k)]
        scratch += [
            pltpu.SemaphoreType.DMA,
            pltpu.SemaphoreType.DMA,
            pltpu.SemaphoreType.DMA((cycle, 4)),
            pltpu.SemaphoreType.DMA((stacks + 1, cycle, max_pieces)),
            pltpu.SemaphoreType.DMA((2 * (stacks + 1), cycle, max_pieces)),
        ]
        macs = rows * (4 * res_ch * gate + gate * (res_ch + skip_ch))
        hidden, skip = pl.pallas_call(
            functools.partial(wavenet_kernel, n_sp, stacks, cycle),
            out_shape=(pltpu.VMEM((PRE + rows, res_ch), bf16), pltpu.VMEM((rows, skip_ch), f32)),
            in_specs=[hbm] * 6,
            out_specs=(vmem, vmem),
            scratch_shapes=scratch,
            compiler_params=pltpu.CompilerParams(collective_id=0, has_side_effects=True,
                                                 vmem_limit_bytes=VMEM_MIB * 2 ** 20),
            cost_estimate=pl.CostEstimate(flops=2 * macs * stacks * cycle, bytes_accessed=90 * 2 ** 20,
                                          transcendentals=0),
            name="wavenet",
        )(x_seq, w_past, w_now, jnp.transpose(b_conv, (1, 0, 2)), w_res, w_skip)
        return pl.pallas_call(
            head_kernel,
            out_shape=(jax.ShapeDtypeStruct((rows, w_out2.shape[-1]), f32),
                       jax.ShapeDtypeStruct((rows, res_ch), bf16)),
            in_specs=[vmem] * 6,
            out_specs=(hbm, hbm),
            scratch_shapes=[pltpu.VMEM((rows, w_out2.shape[-1]), f32), pltpu.SemaphoreType.DMA((2,))],
            compiler_params=pltpu.CompilerParams(vmem_limit_bytes=8 * 2 ** 20),
            name="head",
        )(hidden, skip, w_out1, b_out1.reshape(1, -1), w_out2, b_out2.reshape(1, -1))

    return jax.shard_map(
        local_stack,
        mesh=mesh,
        in_specs=(row_spec, P(), P(), P(), P(), P(), P(), P(), P(), P()),
        out_specs=(row_spec, row_spec),
        check_vma=False,
    )
```
